32 devices in a mesh: rep: 2 (over x), dp: 16 (over y, z, core).
Axes of the slice: x: 2, y: 2, z: 4, core: 2. Of those that a mesh axis runs over, the one named last changes fastest.
Arguments:
- x: bfloat16 [32, 2048, 896], P(('rep', 'dp')), parts along dimension 0
- dy: bfloat16 [32, 2048, 896], P(('rep', 'dp')), parts along dimension 0
- wq: bfloat16 [2, 896, 896], replicated
- wk: bfloat16 [2, 896, 128], replicated
- wv: bfloat16 [2, 896, 128], replicated
- wo: bfloat16 [2, 896, 896], replicated
- w_gate: bfloat16 [2, 896, 2560], replicated
- w_up: bfloat16 [2, 896, 2560], replicated
- w_down: bfloat16 [2, 2560, 896], replicated
- m_wq: float32 [2, 896, 896], replicated
- m_wk: float32 [2, 896, 128], replicated
- m_wv: float32 [2, 896, 128], replicated
- m_wo: float32 [2, 896, 896], replicated
- m_w_gate: float32 [2, 896, 2560], replicated
- m_w_up: float32 [2, 896, 2560], replicated
- m_w_down: float32 [2, 2560, 896], replicated
- v_wq: float32 [2, 896, 896], replicated
- v_wk: float32 [2, 896, 128], replicated
- v_wv: float32 [2, 896, 128], replicated
- v_wo: float32 [2, 896, 896], replicated
- v_w_gate: float32 [2, 896, 2560], replicated
- v_w_up: float32 [2, 896, 2560], replicated
- v_w_down: float32 [2, 2560, 896], replicated
Outputs:
- output 1: bfloat16 [4, 896, 896], P('rep'), parts along dimension 0
- output 2: bfloat16 [4, 896, 128], P('rep'), parts along dimension 0
- output 3: bfloat16 [4, 896, 128], P('rep'), parts along dimension 0
- output 4: bfloat16 [4, 896, 896], P('rep'), parts along dimension 0
- output 5: bfloat16 [4, 896, 2560], P('rep'), parts along dimension 0
- output 6: bfloat16 [4, 896, 2560], P('rep'), parts along dimension 0
- output 7: bfloat16 [4, 2560, 896], P('rep'), parts along dimension 0
- output 8: float32 [4, 896, 896], P('rep'), parts along dimension 0
- output 9: float32 [4, 896, 128], P('rep'), parts along dimension 0
- output 10: float32 [4, 896, 128], P('rep'), parts along dimension 0
- output 11: float32 [4, 896, 896], P('rep'), parts along dimension 0
- output 12: float32 [4, 896, 2560], P('rep'), parts along dimension 0
- output 13: float32 [4, 896, 2560], P('rep'), parts along dimension 0
- output 14: float32 [4, 2560, 896], P('rep'), parts along dimension 0
- output 15: float32 [4, 896, 896], P('rep'), parts along dimension 0
- output 16: float32 [4, 896, 128], P('rep'), parts along dimension 0
- output 17: float32 [4, 896, 128], P('rep'), parts along dimension 0
- output 18: float32 [4, 896, 896], P('rep'), parts along dimension 0
- output 19: float32 [4, 896, 2560], P('rep'), parts along dimension 0
- output 20: float32 [4, 896, 2560], P('rep'), parts along dimension 0
- output 21: float32 [4, 2560, 896], P('rep'), parts along dimension 0
There are 2 independent parts. The reference program is written for one: setup_inputs(seed, part) draws one part's arguments, and reference() takes and returns one part's arrays. A program takes and returns all parts, laid end to end along the dimension named above; an argument that names none is the same for every part.
All inputs are finite; a program needn't handle non-finite values.
Results may differ from the reference program's by a relative error of at most 0.024.
Values are sent between devices in bfloat16 or wider.
A program may use at most 2.75 GiB of HBM per device.

```python
import jax
import jax.numpy as jnp
from jax import lax

SEQUENCES = 16
TOKENS = 2048
D = 896
HEADS = 7
KV_HEADS = 1
HEAD = 128
FF = 2560
LAYERS = 2
THETA = 10000
NAMES = ("wq", "wk", "wv", "wo", "w_gate", "w_up", "w_down")
SHAPES = {
    "wq": (LAYERS, D, HEADS * HEAD),
    "wk": (LAYERS, D, KV_HEADS * HEAD),
    "wv": (LAYERS, D, KV_HEADS * HEAD),
    "wo": (LAYERS, HEADS * HEAD, D),
    "w_gate": (LAYERS, D, FF),
    "w_up": (LAYERS, D, FF),
    "w_down": (LAYERS, FF, D),
}


def bump(key, n, height):
    away = (jnp.arange(n, dtype=jnp.int32) - jax.random.randint(key, (), 0, n, jnp.int32)) % n
    return jnp.where(away < n // 8, height, 1.0)


def together(key, own, strength):
    shared = jax.random.normal(key, own.shape[1:], jnp.float32)
    return (own + strength * shared) * lax.rsqrt(1 + strength * strength)


def setup_inputs(seed: int = 0, part: int = 0) -> dict:
    kx, kdy, ka, kb, kz, kf, kh, kl, *keys = jax.random.split(jax.random.key(seed), 8 + 3 * len(NAMES))
    kx, kdy, ka, kb = (jax.random.fold_in(k, part) for k in (kx, kdy, ka, kb))
    kw, km, kv = (keys[i::3] for i in range(3))
    shape = (SEQUENCES, TOKENS, D)
    much_x, much_dy = jax.random.uniform(kz, (2,), jnp.float32, 0.0, 1.0)
    loud = 2.0 ** jax.random.uniform(jax.random.fold_in(kz, 1), (), jnp.float32, -1.0, 2.0)
    layers = 2.0 ** jax.random.uniform(kl, (LAYERS, 1, 1), jnp.float32, -1.0, 1.0)
    times = {"wq": 1.0, "wk": 1.0, "wv": 2.0, "wo": layers, "w_gate": 1.0, "w_up": bump(kh, FF, 4.0), "w_down": layers}
    x = together(ka, jax.random.normal(kx, shape, jnp.float32), much_x) * bump(kf, D, 4.0)
    dy = together(kb, jax.random.normal(kdy, shape, jnp.float32), much_dy)
    drawn = {"x": x.astype(jnp.bfloat16), "dy": (loud * dy * (SEQUENCES * TOKENS) ** -0.5).astype(jnp.bfloat16)}
    for key, name in zip(kw, NAMES, strict=True):
        drawn[name] = (jax.random.normal(key, SHAPES[name], jnp.float32) * SHAPES[name][1] ** -0.5 * times[name]).astype(jnp.bfloat16)
    for key, name in zip(km, NAMES, strict=True):
        drawn[f"m_{name}"] = 0.1 * jax.random.normal(key, SHAPES[name], jnp.float32)
    for key, name in zip(kv, NAMES, strict=True):
        drawn[f"v_{name}"] = jax.random.uniform(key, SHAPES[name], jnp.float32, 0.02, 0.06)
    return drawn


def matmul(a, w):
    return jnp.dot(a, w, preferred_element_type=jnp.float32).astype(jnp.bfloat16)


def normed(h):
    wide = h.astype(jnp.float32)
    scale = lax.rsqrt(jnp.mean(wide**2, -1, keepdims=True) + 1e-6)
    return (wide * scale).astype(jnp.bfloat16)


def turned(t, theta):
    half = t.shape[-1] // 2
    angle = jnp.arange(t.shape[0], dtype=jnp.float32)[:, None] * theta ** (-jnp.arange(half, dtype=jnp.float32) / half)
    cos, sin = jnp.cos(angle)[:, None], jnp.sin(angle)[:, None]
    a, b = t[..., :half].astype(jnp.float32), t[..., half:].astype(jnp.float32)
    return jnp.concatenate([a * cos - b * sin, b * cos + a * sin], -1).astype(jnp.bfloat16)


def seen_by(q, k, v):
    tokens, kv = q.shape[0], k.shape[1]
    q = q.reshape(tokens, kv, -1, q.shape[-1])
    scores = jnp.einsum("tgsd,ugd->gstu", q.astype(jnp.float32), k.astype(jnp.float32)) * q.shape[-1] ** -0.5
    place = jnp.arange(tokens)
    weights = jax.nn.softmax(jnp.where(place[:, None] >= place, scores, -jnp.inf), -1).astype(jnp.bfloat16)
    return jnp.einsum("gstu,ugd->tgsd", weights.astype(jnp.float32), v.astype(jnp.float32)).astype(jnp.bfloat16).reshape(tokens, -1)


def layer(h, w):
    a = normed(h)
    q, k = (turned(matmul(a, w[name]).reshape(h.shape[0], -1, HEAD), THETA) for name in ("wq", "wk"))
    h = h + matmul(seen_by(q, k, matmul(a, w["wv"]).reshape(h.shape[0], -1, HEAD)), w["wo"])
    b = normed(h)
    gate = jnp.dot(b, w["w_gate"], preferred_element_type=jnp.float32)
    up = jnp.dot(b, w["w_up"], preferred_element_type=jnp.float32)
    return h + matmul((jax.nn.silu(gate) * up).astype(jnp.bfloat16), w["w_down"])


def adamw(w, m, v, g):
    m = 0.9 * m + 0.1 * g
    v = 0.95 * v + 0.05 * g * g
    step = m * lax.rsqrt(v + 1e-8) + 0.1 * w
    return (w - 0.02 * step).astype(jnp.bfloat16), m, v


def clipped(gradients, sum_of_squares, count):
    factor = jnp.minimum(1.0, 0.5 * lax.rsqrt(sum_of_squares / count + 1e-30))
    return [g * factor for g in gradients]


def stack(weights, h):
    return lax.scan(lambda h, w: (layer(h, w), None), h, weights)[0]


def reference(x, dy, wq, wk, wv, wo, w_gate, w_up, w_down, m_wq, m_wk, m_wv, m_wo, m_w_gate, m_w_up, m_w_down, v_wq, v_wk, v_wv, v_wo, v_w_gate, v_w_up, v_w_down):
    weights = dict(zip(NAMES, (wq, wk, wv, wo, w_gate, w_up, w_down), strict=True))

    def take(so_far, sequence):
        h, by_y = sequence
        _, back = jax.vjp(stack, weights, h)
        by_weights, by_h = back(by_y)
        return jax.tree.map(lambda total, term: total + term.astype(jnp.float32), so_far, by_weights), by_h

    none_yet = {name: jnp.zeros(w.shape, jnp.float32) for name, w in weights.items()}
    by_weights, by_x = lax.scan(take, none_yet, (x, dy))
    gradients = [by_weights[name].astype(jnp.bfloat16).astype(jnp.float32) for name in NAMES]
    gradients = clipped(gradients, sum(jnp.sum(g * g) for g in gradients), sum(g.size for g in gradients))
    first = (m_wq, m_wk, m_wv, m_wo, m_w_gate, m_w_up, m_w_down)
    second = (v_wq, v_wk, v_wv, v_wo, v_w_gate, v_w_up, v_w_down)
    new = [adamw(weights[name].astype(jnp.float32), m, v, g) for name, m, v, g in zip(NAMES, first, second, gradients, strict=True)]
    return tuple(one[which] for which in range(3) for one in new)
```

```python
import functools

import jax
import jax.numpy as jnp
from jax import lax
from jax.experimental import pallas as pl
from jax.experimental.pallas import tpu as pltpu

NEG = -1e30
HIDDEN = 2 * NEG
LOG2E = 1.4426950408889634
VMEM = 56 * 2**20
KEYS = 512
QUERIES = 512
QUERIES_BACK = 256


def _dot(a, b, ca, cb):
    return lax.dot_general(a, b, (((ca,), (cb,)), ((), ())), preferred_element_type=jnp.float32)


def _blocks(block, iq, bq, bk):
    whole, last = lax.div(iq * bq + 1, bk), lax.div(iq * bq + bq - 1 + bk, bk)
    lax.fori_loop(0, whole, lambda j, _: block(j, False), None)
    lax.fori_loop(whole, last, lambda j, _: block(j, True), None)


def _gap(bk, cols, bq):
    return lax.rem(lax.broadcasted_iota(jnp.int32, (bk, cols), 1), bq) - lax.broadcasted_iota(jnp.int32, (bk, cols), 0)


def _row(ref):
    return jnp.concatenate([ref[0, 0, n : n + 1, :] for n in range(ref.shape[2])], axis=1)


def _forward(q_ref, k_ref, v_ref, o_ref, lse_ref, top_s, mix_s, gap_s, *, scale, bk, wide):
    g, bq, d = q_ref.shape[2:]
    cols, low, iq = g * bq, k_ref.dtype, pl.program_id(0)
    e = scale * LOG2E
    pieces = range(0, cols, wide)

    @pl.when(iq == 0)
    def _():
        gap_s[...] = _gap(bk, cols, bq)

    top_s[...] = jnp.full_like(top_s, NEG)
    mix_s[...] = jnp.zeros_like(mix_s)
    ones = jnp.ones((8, bk), low)

    def block(j, masked):
        here = pl.ds(j * bk, bk)
        scores = [_dot(k_ref[0, 0, here, :], q_ref[0, 0].reshape(cols, d)[at : at + wide, :], 1, 1) for at in pieces]
        ok = gap_s[...] >= j * bk - iq * bq if masked else None
        weights, keeps = [], []
        for at, s in zip(pieces, scores):
            if masked:
                s = jnp.where(ok[:, at : at + wide], s, HIDDEN)
            old = top_s[:, at : at + wide]
            top = jnp.maximum(old, s.max(axis=0, keepdims=True))
            top_s[:, at : at + wide] = top
            weights.append(jnp.exp2((s - top) * e).astype(low))
            keeps.append(jnp.exp2((old - top) * e))
        for at, p, keep in zip(pieces, weights, keeps):
            values = jnp.concatenate([v_ref[0, 0, here, :].T, ones], axis=0)
            mix_s[:, at : at + wide] = mix_s[:, at : at + wide] * keep + _dot(values, p, 1, 0)

    _blocks(block, iq, bq, bk)
    top, total = top_s[...], mix_s[d : d + 1, :]
    o_ref[0, 0] = (mix_s[:d, :] * (1 / total)).T.reshape(g, bq, d).astype(o_ref.dtype)
    lse = top * scale + jnp.log(total)
    for n in range(g):
        lse_ref[0, 0, n : n + 1, :] = lse[:, n * bq : (n + 1) * bq]


def _cost(h, s, width, arrays):
    return pl.CostEstimate(flops=2 * h * s * s * width, transcendentals=h * s * s, bytes_accessed=sum(a.size * a.dtype.itemsize for a in arrays))


def _specs(g, bq, s, d):
    return (pl.BlockSpec((1, 1, g, bq, d), lambda i: (0, 0, 0, i, 0)), pl.BlockSpec((1, 1, g, bq), lambda i: (0, 0, 0, i)),
            pl.BlockSpec((1, 1, s, d), lambda i: (0, 0, 0, 0)))


def attend(q, k, v):
    _, g, s, d = q.shape
    bq, bk = QUERIES, KEYS
    queries, stats, keys = _specs(g, bq, s, d)
    out, lse = pl.pallas_call(
        functools.partial(_forward, scale=d**-0.5, bk=bk, wide=512),
        grid=(s // bq,),
        in_specs=[queries, keys, keys],
        out_specs=[queries, stats],
        scratch_shapes=[pltpu.VMEM((1, g * bq), jnp.float32), pltpu.VMEM((d + 8, g * bq), jnp.float32), pltpu.VMEM((bk, g * bq), jnp.int32)],
        out_shape=[jax.ShapeDtypeStruct(q[None].shape, q.dtype), jax.ShapeDtypeStruct(q[None].shape[:-1], jnp.float32)],
        compiler_params=pltpu.CompilerParams(dimension_semantics=("arbitrary",), vmem_limit_bytes=VMEM),
        cost_estimate=_cost(g, s, 2 * d, [q, q, k, v]),
        name="attend",
    )(q[None], k, v)
    return out[0], lse[0]


def row_dot(d_out, out):
    return (d_out.astype(jnp.float32) * out.astype(jnp.float32)).sum(-1)


def _backward(q_ref, k_ref, v_ref, do_ref, lse_ref, delta_ref, dq_ref, dk_ref, dv_ref, dq_s, dk_s, dv_s, gap_s, *, scale, bk, wide):
    g, bq, d = q_ref.shape[2:]
    cols, low, iq = g * bq, q_ref.dtype, pl.program_id(0)
    e = scale * LOG2E
    pieces = range(0, cols, wide)

    @pl.when(iq == 0)
    def _():
        gap_s[...] = _gap(bk, cols, bq)
        dk_s[...] = jnp.zeros_like(dk_s)
        dv_s[...] = jnp.zeros_like(dv_s)

    dq_s[...] = jnp.zeros_like(dq_s)
    lses, deltas = _row(lse_ref) * LOG2E, _row(delta_ref)

    def block(j, masked):
        here = pl.ds(j * bk, bk)
        qs = [q_ref[0, 0].reshape(cols, d)[at : at + wide, :] for at in pieces]
        dos = [do_ref[0, 0].reshape(cols, d)[at : at + wide, :] for at in pieces]
        scores = [_dot(k_ref[0, 0, here, :], x, 1, 1) for x in qs]
        dps = [_dot(v_ref[0, 0, here, :], x, 1, 1) for x in dos]
        ok = gap_s[...] >= j * bk - iq * bq if masked else None
        for n, at in enumerate(pieces):
            p = jnp.exp2(scores[n] * e - lses[:, at : at + wide])
            if masked:
                p = jnp.where(ok[:, at : at + wide], p, 0.0)
            ds = (p * (dps[n] - deltas[:, at : at + wide])).astype(low)
            dv_s[here, :] += _dot(p.astype(low), dos[n], 1, 0)
            dk_s[here, :] += _dot(ds, qs[n], 1, 0)
            dq_s[:, at : at + wide] += _dot(k_ref[0, 0, here, :].T, ds, 1, 0)

    _blocks(block, iq, bq, bk)
    dq_ref[0, 0] = (dq_s[...] * scale).T.reshape(g, bq, d).astype(dq_ref.dtype)

    @pl.when(iq == pl.num_programs(0) - 1)
    def _():
        dk_ref[0, 0] = (dk_s[...] * scale).astype(dk_ref.dtype)
        dv_ref[0, 0] = dv_s[...].astype(dv_ref.dtype)


def attend_bwd(q, k, v, d_out, lse, delta):
    _, g, s, d = q.shape
    bq, bk = QUERIES_BACK, KEYS
    queries, stats, keys = _specs(g, bq, s, d)
    dq, dk, dv = pl.pallas_call(
        functools.partial(_backward, scale=d**-0.5, bk=bk, wide=256),
        grid=(s // bq,),
        in_specs=[queries, keys, keys, queries, stats, stats],
        out_specs=[queries, keys, keys],
        scratch_shapes=[pltpu.VMEM((d, g * bq), jnp.float32), pltpu.VMEM((s, d), jnp.float32), pltpu.VMEM((s, d), jnp.float32),
                        pltpu.VMEM((bk, g * bq), jnp.int32)],
        out_shape=[jax.ShapeDtypeStruct(q[None].shape, q.dtype), jax.ShapeDtypeStruct(k.shape, q.dtype), jax.ShapeDtypeStruct(v.shape, q.dtype)],
        compiler_params=pltpu.CompilerParams(dimension_semantics=("arbitrary",), vmem_limit_bytes=VMEM),
        cost_estimate=_cost(g, s, 5 * d, [q, q, k, k, v, v, d_out]),
        name="attend_bwd",
    )(q[None], k, v, d_out[None], lse[None], delta[None])
    return dq[0], dk, dv


from jax.sharding import PartitionSpec as P

HEAD = 128
THETA = 10000
NAMES = ("wq", "wk", "wv", "wo", "w_gate", "w_up", "w_down")
TILE = 512
PART = 512
BF, F32 = jnp.bfloat16, jnp.float32


def _params():
    return pltpu.CompilerParams(dimension_semantics=("arbitrary",), vmem_limit_bytes=VMEM)


def _tokens(width):
    return pl.BlockSpec((TILE, width), lambda i: (i, 0))


def _heads(heads):
    return pl.BlockSpec((heads, TILE, HEAD), lambda i: (0, i, 0))


def _whole(w, number):
    return pl.BlockSpec((None, *w.shape[1:]), lambda i: (number, 0, 0), pipeline_mode=pl.Buffered(1))


def _flops(tokens, *weights):
    flops = sum(2 * tokens * w.shape[1] * w.shape[2] for w in weights)
    return pl.CostEstimate(flops=flops, transcendentals=0, bytes_accessed=tokens * 8192 + sum(2 * w.shape[1] * w.shape[2] for w in weights))


def _normed(wide):
    scale = lax.rsqrt(jnp.mean(wide**2, -1, keepdims=True) + 1e-6)
    return wide * scale, scale


def _lined(ref):
    return jnp.concatenate([ref[n] for n in range(ref.shape[0])], axis=1)


def _norm_back(by, n, scale):
    return scale * (by - n * jnp.mean(by * n, -1, keepdims=True))


def _project(h_ref, wq_ref, wk_ref, wv_ref, cos_ref, sin_ref, q_ref, k_ref, v_ref):
    a = _normed(h_ref[...].astype(F32))[0].astype(BF)
    cos, sin = cos_ref[...], sin_ref[...]

    def turn(t):
        t = t.astype(BF).astype(F32)
        return (t * cos + pltpu.roll(t, HEAD // 2, 1) * sin).astype(BF)

    q = _dot(a, wq_ref[...], 1, 0)
    for n in range(q_ref.shape[0]):
        q_ref[n] = turn(q[:, n * HEAD : (n + 1) * HEAD])
    k_ref[0] = turn(_dot(a, wk_ref[...], 1, 0))
    v_ref[0] = _dot(a, wv_ref[...], 1, 0).astype(BF)


def project(h, wq, wk, wv, cos, sin, number):
    tokens, d = h.shape
    heads = wq.shape[2] // HEAD
    shape = lambda n: jax.ShapeDtypeStruct((n, tokens, HEAD), BF)
    return pl.pallas_call(
        _project,
        grid=(tokens // TILE,),
        in_specs=[_tokens(d), _whole(wq, number), _whole(wk, number), _whole(wv, number), _tokens(HEAD), _tokens(HEAD)],
        out_specs=[_heads(heads), _heads(1), _heads(1)],
        out_shape=[shape(heads), shape(1), shape(1)],
        compiler_params=_params(),
        cost_estimate=_flops(tokens, wq, wk, wv),
        name="project",
    )(h, wq, wk, wv, cos, sin)


def _finish(h_ref, o_ref, wo_ref, wg_ref, wu_ref, wd_ref, h1_ref, h2_ref, line_ref):
    o = _lined(o_ref)
    line_ref[...] = o
    h1 = h_ref[...] + _dot(o, wo_ref[...], 1, 0).astype(BF)
    h1_ref[...] = h1
    b = _normed(h1.astype(F32))[0].astype(BF)
    total = None
    for at in range(0, wg_ref.shape[1], PART):
        cut = slice(at, at + PART)
        gate, up = _dot(b, wg_ref[:, cut], 1, 0), _dot(b, wu_ref[:, cut], 1, 0)
        s = (gate * jax.nn.sigmoid(gate) * up).astype(BF)
        one = _dot(s, wd_ref[cut, :], 1, 0)
        total = one if total is None else total + one
    h2_ref[...] = h1 + total.astype(BF)


def finish(h, o, wo, wg, wu, wd, number):
    tokens, d = h.shape
    state = jax.ShapeDtypeStruct((tokens, d), BF)
    return pl.pallas_call(
        _finish,
        grid=(tokens // TILE,),
        in_specs=[_tokens(d), _heads(o.shape[0]), *(_whole(w, number) for w in (wo, wg, wu, wd))],
        out_specs=[_tokens(d), _tokens(d), _tokens(wo.shape[1])],
        out_shape=[state, state, jax.ShapeDtypeStruct((tokens, wo.shape[1]), BF)],
        compiler_params=_params(),
        cost_estimate=_flops(tokens, wo, wg, wu, wd),
        name="finish",
    )(h, o, wo, wg, wu, wd)


def _unfinish(h1_ref, dy_ref, wo_ref, wg_ref, wu_ref, wd_ref, dgu_ref, s_ref, b_ref, dh_ref, do_ref):
    n, scale = _normed(h1_ref[...].astype(F32))
    b = n.astype(BF)
    b_ref[...] = b
    dy = dy_ref[...]
    total = None
    for at in range(0, wg_ref.shape[1], PART):
        cut = slice(at, at + PART)
        gate, up = _dot(b, wg_ref[:, cut], 1, 0), _dot(b, wu_ref[:, cut], 1, 0)
        ds = _dot(dy, wd_ref[cut, :], 1, 1).astype(BF).astype(F32)
        sig = jax.nn.sigmoid(gate)
        act = gate * sig
        s_ref[:, cut] = (act * up).astype(BF)
        du = (ds * act).astype(BF)
        dg = (ds * up * (sig * (1.0 + gate * (1.0 - sig)))).astype(BF)
        dgu_ref[:, cut] = dg
        dgu_ref[:, wg_ref.shape[1] + at : wg_ref.shape[1] + at + PART] = du
        one = _dot(dg, wg_ref[:, cut], 1, 1) + _dot(du, wu_ref[:, cut], 1, 1)
        total = one if total is None else total + one
    dh = (dy.astype(F32) + _norm_back(total, n, scale)).astype(BF)
    dh_ref[...] = dh
    do = _dot(dh, wo_ref[...], 1, 1).astype(BF)
    for i in range(do_ref.shape[0]):
        do_ref[i] = do[:, i * HEAD : (i + 1) * HEAD]


def unfinish(h1, dy, wo, wg, wu, wd, number):
    tokens, d = h1.shape
    ff, heads = wg.shape[2], wo.shape[1] // HEAD
    shape = lambda width: jax.ShapeDtypeStruct((tokens, width), BF)
    return pl.pallas_call(
        _unfinish,
        grid=(tokens // TILE,),
        in_specs=[_tokens(d), _tokens(d), *(_whole(w, number) for w in (wo, wg, wu, wd))],
        out_specs=[_tokens(2 * ff), _tokens(ff), _tokens(d), _tokens(d), _heads(heads)],
        out_shape=[shape(2 * ff), shape(ff), shape(d), shape(d), jax.ShapeDtypeStruct((heads, tokens, HEAD), BF)],
        compiler_params=_params(),
        cost_estimate=_flops(tokens, wo, wg, wg, wu, wu, wd),
        name="unfinish",
    )(h1, dy, wo, wg, wu, wd)


def _unproject(last, dq_ref, dk_ref, dv_ref, h_ref, cos_ref, sin_ref, *rest):
    cos, sin = cos_ref[...], sin_ref[...]

    def turn(t):
        t = t.astype(F32)
        return (t * cos - pltpu.roll(t, HEAD // 2, 1) * sin).astype(BF)

    n, scale = _normed(h_ref[...].astype(F32))
    every = jnp.concatenate([turn(dq_ref[i]) for i in range(dq_ref.shape[0])] + [turn(dk_ref[0]), dv_ref[0]], axis=1)
    if last:
        all_ref, a_ref = rest
    else:
        dh1_ref, wq_ref, wk_ref, wv_ref, all_ref, a_ref, dh_ref = rest
        w = jnp.concatenate([wq_ref[...], wk_ref[...], wv_ref[...]], axis=1)
        da = _dot(every, w, 1, 1)
        dh_ref[...] = (dh1_ref[...].astype(F32) + _norm_back(da, n, scale)).astype(BF)
    all_ref[...] = every
    a_ref[...] = n.astype(BF)


def unproject(dq, dk, dv, h, cos, sin, dh1, wq, wk, wv, number):
    tokens, d = h.shape
    width = (dq.shape[0] + 2) * HEAD
    last = number == 0
    given, specs = [dq, dk, dv, h, cos, sin], [_heads(dq.shape[0]), _heads(1), _heads(1), _tokens(d), _tokens(HEAD), _tokens(HEAD)]
    shapes = [jax.ShapeDtypeStruct((tokens, width), BF), jax.ShapeDtypeStruct((tokens, d), BF)]
    if not last:
        given += [dh1, wq, wk, wv]
        specs += [_tokens(d), _whole(wq, number), _whole(wk, number), _whole(wv, number)]
        shapes += [jax.ShapeDtypeStruct((tokens, d), BF)]
    return pl.pallas_call(
        functools.partial(_unproject, last),
        grid=(tokens // TILE,),
        in_specs=specs,
        out_specs=[_tokens(s.shape[1]) for s in shapes],
        out_shape=shapes,
        compiler_params=_params(),
        cost_estimate=_flops(tokens, wq, wk, wv),
        name="unproject",
    )(*given)


class Group:
    def __init__(self, mesh):
        self.zs = mesh.shape["dp"] // 4
        self.place = lax.axis_index("dp")

    def bit(self, step):
        at = self.place
        if step == "core":
            return at % 2
        if step == "y":
            return at // (2 * self.zs)
        z = (at // 2) % self.zs
        return z % 2 if step == "near" else z // 2

    def exchange(self, x, step):
        flip = {"core": 1, "near": 2, "far": 4, "y": 2 * self.zs}[step]
        return lax.ppermute(x, "dp", [(i, i ^ flip) for i in range(4 * self.zs)])

    def relative(self, order):
        at = 0
        for step in order:
            at = 2 * at + self.bit(step)
        return at

    def total(self, x, order):
        for step in order:
            x = x + self.exchange(x, step)
        return x


class Line:
    def __init__(self):
        self.live = {}

    def cut(self):
        names = list(self.live)
        self.live = dict(zip(names, lax.optimization_barrier(tuple(self.live[n] for n in names)), strict=True))


class Chain:
    def __init__(self, group, line, name, order):
        self.group, self.line, self.name, self.order = group, line, name, order
        self.at, self.flying = 0, None

    def begin(self, g):
        self.line.live[self.name] = g
        self.send()

    def _half(self, x, bit):
        half = x.shape[0] // 2
        return lax.dynamic_slice_in_dim(x, bit * half, half, 0)

    def send(self):
        x, steps = self.line.live[self.name], len(self.order)
        if self.at < steps:
            step = self.order[self.at]
            self.flying = self.group.exchange(self._half(x, 1 - self.group.bit(step)), step)
        else:
            self.flying = self.group.exchange(x, self.order[2 * steps - 1 - self.at])

    def land(self):
        x, got, steps = self.line.live[self.name], self.flying, len(self.order)
        if self.at < steps:
            kept = self._half(x, self.group.bit(self.order[self.at]))
            new = self.line.live[self.name] = (kept.astype(F32) + got.astype(F32)).astype(BF)
            if self.at == steps - 1:
                self.line.live[self.name + "_squares"] = jnp.sum(jnp.square(new.astype(F32)))
        elif self.at < 2 * steps - 1:
            self.line.live[self.name] = jnp.concatenate([x, got], axis=0)
        else:
            self.line.live[self.name + "_other"] = got
        self.at += 1

    def go(self):
        self.land()
        if self.at < 2 * len(self.order):
            self.send()

    def take(self):
        return self.line.live.pop(self.name), self.line.live.pop(self.name + "_other")


Y_FIRST = ("core", "y", "near", "far")
Z_FIRST = ("core", "near", "far", "y")


def _adamw(places, n_g, count, pos_ref, f_ref, *refs):
    f = f_ref[0]
    j = pl.program_id(0)
    halves = n_g[0]
    gs, rest = refs[: sum(n_g)], refs[sum(n_g) :]
    n_w = len(places)
    outs = rest[-3 * n_w :]
    for index, (which, at) in enumerate(places):
        w_ref, m_ref, v_ref = rest[3 * index : 3 * index + 3]
        w_out, m_out, v_out = (outs[group * n_w + index] for group in range(3))
        cut = slice(at, at + w_ref.shape[1])

        def update(g_ref, w_ref=w_ref, m_ref=m_ref, v_ref=v_ref, w_out=w_out, m_out=m_out, v_out=v_out, cut=cut):
            g = g_ref[:, cut].astype(F32) * f
            m = 0.9 * m_ref[...] + 0.1 * g
            v = 0.95 * v_ref[...] + 0.05 * g * g
            w = w_ref[...].astype(F32)
            step = m * lax.rsqrt(v + 1e-8) + 0.1 * w
            w_out[...] = (w - 0.02 * step).astype(BF)
            m_out[...] = m
            v_out[...] = v

        if halves == 1:
            update(gs[which])
        else:
            for half in range(2):
                pl.when((j >= count // 2) == bool(half))(functools.partial(update, gs[2 * which + half]))


def adamw(gradients, places, arrays, so_far, number, order, position, factor, count):
    half = count // 2
    given, specs = [], []
    place = {"core": 0, "near": 1, "far": 2, "y": 3}

    def holder(j):
        return sum(((j >> (len(order) - 1 - n)) & 1) << place[step] for n, step in enumerate(order))

    for g in gradients:
        if len(g) == 1:
            given += g
            specs += [pl.BlockSpec((g[0].shape[0] // count, g[0].shape[1]), lambda j, *_: (holder(j), 0))]
        else:
            rows, width = g[0].shape[0] // half, g[0].shape[1]
            given += g
            specs += [pl.BlockSpec((rows, width), lambda j, *_: (jnp.minimum(j, half - 1), 0)),
                      pl.BlockSpec((rows, width), lambda j, *_: (jnp.maximum(j - half, 0), 0))]
    relative = len(gradients[0]) == 2
    outs, shapes = [[], [], []], [[], [], []]
    for three in arrays:
        for n, t in enumerate(three):
            spec = pl.BlockSpec((None, t.shape[1] // count, t.shape[2]), lambda j, pos, _: (number, j ^ pos[0] if relative else j, 0))
            given.append(t)
            specs.append(spec)
            outs[n].append(spec)
            shapes[n].append(jax.ShapeDtypeStruct(t.shape, t.dtype))
    alias = {}
    if so_far is not None:
        for n, t in enumerate(so_far):
            alias[2 + len(given)] = n
            given.append(t)
            specs.append(pl.BlockSpec(memory_space=pl.ANY))
    size = sum(a[0].size for a in arrays) // arrays[0][0].shape[0]
    return pl.pallas_call(
        functools.partial(_adamw, places, [len(g) for g in gradients], count),
        grid_spec=pltpu.PrefetchScalarGridSpec(num_scalar_prefetch=2, grid=(count,), in_specs=specs, out_specs=sum(outs, [])),
        out_shape=sum(shapes, []),
        input_output_aliases=alias,
        compiler_params=pltpu.CompilerParams(dimension_semantics=("arbitrary",), vmem_limit_bytes=VMEM),
        cost_estimate=pl.CostEstimate(flops=200 * size, transcendentals=0, bytes_accessed=22 * size),
        name="adamw",
    )(position.reshape(1), factor.reshape(1), *given)


def by_weight(a, g):
    return _dot(a, g, 0, 0).astype(BF)


def solution(mesh):
    def step(x, dy, *arrays):
        weights, m, v = (arrays[i : i + 7] for i in (0, 7, 14))
        wq, wk, wv, wo, wg, wu, wd = weights
        layers, count = wq.shape[0], mesh.shape["dp"]
        group = Group(mesh)
        tokens = x.shape[1]
        half = HEAD // 2
        angle = jnp.arange(tokens, dtype=F32)[:, None] * THETA ** (-jnp.arange(half, dtype=F32) / half)
        cos, sin = jnp.cos(angle), jnp.sin(angle)
        cos, sin = jnp.concatenate([cos, cos], 1), jnp.concatenate([-sin, sin], 1)

        h, kept = x[0], []
        for number in range(layers):
            q, k, vv = project(h, wq, wk, wv, cos, sin, number)
            o, lse = attend(q[None], k[None], vv[None])
            h1, h2, side = finish(h, o[0], wo, wg, wu, wd, number)
            kept.append((h, q, k, vv, o, lse, h1, side))
            h = h2

        line = Line()
        live = lambda name: line.live[name]
        orders = {"qkv": Z_FIRST, "wo": Z_FIRST, "wgu": Y_FIRST, "wd": Y_FIRST}
        chains = {f"{name}{n}": Chain(group, line, f"{name}{n}", order) for name, order in orders.items() for n in range(layers)}

        def go(*names):
            for name in names:
                chains[name].go()
            line.cut()

        def land(*names):
            for name in names:
                chains[name].land()
            line.cut()

        def mlp_back(n, by_h):
            dgu, s, b, dh1, do = unfinish(kept[n][6], by_h, wo, wg, wu, wd, n)
            line.live.update(dgu=dgu, s=s, b=b, dh1=dh1, do=do, by_h=by_h)
            line.cut()

        def gradient(name, n):
            pairs = {"wd": ("s", "by_h"), "wgu": ("b", "dgu"), "qkv": ("a", "every")}
            a, g = (kept[n][7], live("dh1")) if name == "wo" else map(live, pairs[name])
            chains[f"{name}{n}"].begin(by_weight(a, g))
            for gone in {"wd": ("s",), "wgu": ("dgu", "b"), "qkv": ("a", "every")}.get(name, ()):
                line.live.pop(gone)
            if name == "wo":
                line.live["delta"] = row_dot(live("do")[None], kept[n][4])
            line.cut()

        def attention_back(n):
            h, q, k, vv, o, lse, h1, side = kept[n]
            dq, dk, dv = attend_bwd(q[None], k[None], vv[None], line.live.pop("do")[None], lse, line.live.pop("delta"))
            line.live.update(dq=dq, dk=dk, dv=dv)
            line.cut()

        def project_back(n):
            dq, dk, dv = (line.live.pop(t)[0] for t in ("dq", "dk", "dv"))
            every, a, *more = unproject(dq, dk, dv, kept[n][0], cos, sin, line.live.pop("dh1"), wq, wk, wv, n)
            line.live.update(every=every, a=a)
            line.live.pop("by_h")
            if more:
                line.live["next"] = more[0]
            line.cut()

        got = {}

        def gather(*names):
            for name in names:
                got[name] = lax.all_gather(line.live.pop(name), "dp", axis=0, tiled=True)

        mlp_back(1, dy[0])
        gradient("wd", 1)
        gradient("wgu", 1)
        go("wd1")
        gradient("wo", 1)
        go("wgu1")
        attention_back(1)
        go("wd1", "wo1", "wgu1")
        project_back(1)
        gradient("qkv", 1)
        go("wd1")
        mlp_back(0, line.live.pop("next"))
        go("wgu1", "wo1", "qkv1")
        land("wd1")
        gather("wd1")
        gradient("wd", 0)
        go("qkv1", "wo1")
        gradient("wgu", 0)
        land("wgu1")
        gather("wgu1")
        go("wd0", "qkv1", "wo1")
        gradient("wo", 0)
        go("qkv1")
        go("wgu0")
        attention_back(0)
        go("wd0", "wo0", "wgu0")
        project_back(0)
        gradient("qkv", 0)
        go("wgu0")
        go("wd0", "wo0", "qkv0")
        go("wo0", "qkv0")
        land("wd0")
        gather("wd0")
        go("wo0", "qkv0")
        land("wgu0")
        gather("wgu0")
        go("qkv0")
        squares = sum(line.live.pop(f"{name}{n}_squares") for name in orders for n in range(layers))
        line.live["squares"] = group.total(jnp.full((8, 128), squares, F32), Y_FIRST)
        attending = ("wo0", "qkv0", "wo1", "qkv1")
        go(*attending)
        size = sum(w.size for w in weights)
        line.live["factor"] = jnp.minimum(1.0, 0.5 * lax.rsqrt(line.live.pop("squares")[0, 0] / size + 1e-30))
        line.cut()

        new = {}

        def update(names, gradients, places, n):
            indices = [NAMES.index(name) for name in names]
            three = [(weights[i], m[i], v[i]) for i in indices]
            gathered = [(live(name),) if f"{name}_other" not in line.live else (live(name), live(f"{name}_other")) for name in gradients]
            so_far = [new[what, i] for what in range(3) for i in indices] if (0, indices[0]) in new else None
            order = orders[gradients[0][:-1]]
            out = adamw(gathered, places, three, so_far, n, order, group.relative(order), live("factor"), count)
            for what in range(3):
                for at, i in enumerate(indices):
                    new[what, i] = out[what * len(indices) + at]
            line.live["mark"] = new[0, indices[0]]
            line.cut()
            new[0, indices[0]] = line.live.pop("mark")

        kv, width, ff = wk.shape[2], wq.shape[2], wg.shape[2]
        heads, places = ("wq", "wk", "wv", "wo"), ((0, 0), (0, width), (0, width + kv), (1, 0))
        line.live["wd1"] = got["wd1"]
        update(("w_down",), ("wd1",), ((0, 0),), 1)
        line.live["wgu1"] = got["wgu1"]
        go(*attending)
        update(("w_gate", "w_up"), ("wgu1",), ((0, 0), (0, ff)), 1)
        go(*attending)
        land(*attending)
        update(heads, ("qkv1", "wo1"), places, 1)
        update(heads, ("qkv0", "wo0"), places, 0)
        line.live["wd0"] = got["wd0"]
        update(("w_down",), ("wd0",), ((0, 0),), 0)
        line.live["wgu0"] = got["wgu0"]
        update(("w_gate", "w_up"), ("wgu0",), ((0, 0), (0, ff)), 0)
        return tuple(new[what, i] for what in range(3) for i in range(7))

    states, all_of = P(("rep", "dp"), None, None), P(None, None, None)
    return jax.shard_map(
        step,
        mesh=mesh,
        in_specs=(states, states) + (all_of,) * 21,
        out_specs=(P("rep", None, None),) * 21,
        check_vma=False,
    )
```
